32 devices in a mesh: parts: 2 (over y), rng: 8 (over z, x), chan: 2 (over core).
Axes of the slice: x: 2, y: 2, z: 4, core: 2. Of those that a mesh axis runs over, the one named last changes fastest.
Arguments:
- snapshots: bfloat16 [8, 2, 16384, 192], P('parts', None, 'rng', 'chan'), parts along dimension 0, may hold values from -24 to 24
- train_gates: int32 [8, 128], P('parts', 'rng'), parts along dimension 0, may hold values from 0 to 2047
- guard_keep: int32 [8, 128], P('parts', 'rng'), parts along dimension 0, may hold values 0 or 1
- beam_cells: int32 [8, 16], P('parts'), parts along dimension 0, may hold values from 0 to 767
Outputs:
- beam_out: bfloat16 [8, 2, 16, 16384], P('parts', None, None, ('rng', 'chan')), parts along dimension 0
- weights: float32 [8, 16, 384], P('parts'), parts along dimension 0
The draws below stay inside these ranges and needn't reach their ends.
There are 2 independent parts, one for each index of `parts`. The reference program is written for one: setup_inputs(seed, part) draws one part's arguments, and reference() takes and returns one part's arrays. A program takes and returns all parts, laid end to end along the dimension named above; each array names one. Nothing has to cross between parts.
Inputs may be any that keep to these rules, and one draw needn't show every extreme that they name: `train_gates`: an offset into the 2048 gates of the range group that holds the entry. `beam_cells`: angle cell times 12 plus Doppler cell.
All inputs are finite; a program needn't handle non-finite values. No bound on the sum of `guard_keep` on one device may be relied on, other than what follows from the above.
Results may differ from the reference program's by a relative error of at most 0.01225.
Values may be sent and summed in bfloat16 or wider, within the bound.
A program may use at most 64 MiB of HBM per device.

```python
import math
import jax
import jax.numpy as jnp
from jax import lax

ELEM = 16
PULSE = 12
CH = 192
BEAMS = 16
ANGLES = 64
NB = 4
GATES_DEV = 2048
TRAIN_DEV = 16
GATES = 16384
TRAIN = 128


def rotate_sum(amplitude, heading):
    real_part = jnp.einsum('bgts,bgsc->bgtc', amplitude[:, 0], heading[:, 0]) - jnp.einsum('bgts,bgsc->bgtc', amplitude[:, 1], heading[:, 1])
    imag_part = jnp.einsum('bgts,bgsc->bgtc', amplitude[:, 0], heading[:, 1]) + jnp.einsum('bgts,bgsc->bgtc', amplitude[:, 1], heading[:, 0])
    return jnp.stack([real_part, imag_part], axis=1)


def source_powers(jammer_power, spread_total, spread_count, decades):
    steps = jnp.arange(spread_count, dtype=jnp.float32) / (spread_count - 1)
    spread = jnp.exp(-math.log(10.0) * decades * steps)
    spread = spread * (spread_total / jnp.sum(spread))
    return jnp.concatenate([jnp.full((1,), jammer_power, jnp.float32), spread])


def draw_snapshots(key, part):
    group_count = GATES // GATES_DEV
    local_count = 2
    spread_count = 40
    shared_count = spread_count + 1
    keys = jax.random.split(key, 5)
    shape = (NB, 2, group_count, GATES_DEV, CH)
    rising = 4.0 + 8.0 * jnp.arange(group_count, dtype=jnp.float32) / max(group_count - 1, 1)
    level = (rising / 4.0)[None, None, :, None, None]
    local_amp = jax.random.truncated_normal(keys[1], -3.0, 3.0, (NB, 2, group_count, GATES_DEV, local_count), jnp.float32)
    local_amp = local_amp * jnp.sqrt(0.5 * level)
    local_head = jax.random.truncated_normal(keys[2], -3.0, 3.0, (NB, 2, group_count, local_count, CH), jnp.float32) * math.sqrt(0.5)
    noise = jax.random.truncated_normal(keys[0], -4.0, 4.0, shape, jnp.float32) * 0.25
    local_part = rotate_sum(local_amp, local_head)
    powers = source_powers(10.0, 2.0, spread_count, 3.0)
    shared_amp = jax.random.truncated_normal(keys[3], -3.0, 3.0, (NB, 2, group_count, GATES_DEV, shared_count), jnp.float32)
    shared_amp = shared_amp * jnp.sqrt(0.5 * powers)[None, None, None, None, :] * jnp.sqrt(level)
    phase = jax.random.uniform(keys[4], (NB, 1, 1, shared_count, CH), jnp.float32, -math.pi, math.pi)
    shared_head = jnp.concatenate([jnp.cos(phase), jnp.sin(phase)], axis=1)
    shared_head = jnp.broadcast_to(shared_head, (NB, 2, group_count, shared_count, CH))
    total = noise + local_part + rotate_sum(shared_amp, shared_head)
    total = jnp.clip(total, -24.0, 24.0)
    return total.reshape(NB, 2, GATES, CH).astype(jnp.bfloat16)


def place_ends(array, key, smallest, largest):
    longest = array.shape.index(max(array.shape))
    spots = []
    for shift in (0, 1):
        where = [jax.random.randint(jax.random.fold_in(key, axis), (), 0, length) for axis, length in enumerate(array.shape)]
        where[longest] = (where[longest] + shift) % array.shape[longest]
        spots.append(tuple(where))
    return array.at[spots[0]].set(smallest).at[spots[1]].set(largest)


def setup_inputs(seed: int = 0, part: int = 0) -> dict:
    arg_keys = jax.random.split(jax.random.key(seed), 5)
    part_splits = jax.random.split(jax.random.fold_in(arg_keys[4], part), 5)
    return {
        "snapshots": draw_snapshots(jax.random.fold_in(jax.random.fold_in(arg_keys[4], part), 71), part),
        "train_gates": place_ends(jax.random.randint(part_splits[1], (NB, TRAIN), 0, GATES_DEV), jax.random.fold_in(part_splits[1], 1), 0, GATES_DEV - 1).astype(jnp.int32),
        "guard_keep": place_ends((jax.random.randint(part_splits[2], (NB, TRAIN), 0, 4) < 3).astype(jnp.int32), jax.random.fold_in(part_splits[2], 1), 0, 1),
        "beam_cells": place_ends(jax.random.randint(part_splits[3], (NB, BEAMS), 0, ANGLES * PULSE), jax.random.fold_in(part_splits[3], 1), 0, (ANGLES * PULSE) - 1).astype(jnp.int32),
    }


LOADING = 0.05

def steering(cells):
    angle_cell = (cells // PULSE).astype(jnp.float32)
    doppler_cell = (cells % PULSE).astype(jnp.float32)
    sine_angle = -1.0 + (2.0 * angle_cell + 1.0) / ANGLES
    doppler_freq = (doppler_cell + 0.5) / PULSE - 0.5
    channel = jnp.arange(CH, dtype=jnp.int32)
    element = (channel % ELEM).astype(jnp.float32)
    pulse_index = (channel // ELEM).astype(jnp.float32)
    phases = math.pi * element[None, :] * sine_angle[:, None] + 2.0 * math.pi * pulse_index[None, :] * doppler_freq[:, None]
    norm_scale = 1.0 / math.sqrt(CH)
    return jnp.concatenate([jnp.cos(phases), jnp.sin(phases)], axis=1) * norm_scale

def gram_product(left, right):
    return lax.dot_general(left.astype(jnp.float32), right.astype(jnp.float32), (((0,), (0,)), ((), ())), preferred_element_type=jnp.float32)

def adapt(covariance, steer_vec):
    matrix_order = covariance.shape[0]
    loading = LOADING * jnp.trace(covariance) / matrix_order + 1e-06
    loaded = covariance + loading * jnp.eye(matrix_order, dtype=jnp.float32)
    factor = jnp.linalg.cholesky(loaded)
    forward = lax.linalg.triangular_solve(factor, steer_vec.T, left_side=True, lower=True)
    solved = lax.linalg.triangular_solve(factor, forward, left_side=True, lower=True, transpose_a=True)
    unit_gain = lax.optimization_barrier(jnp.sum(steer_vec.T * solved, axis=0))
    weights = solved / unit_gain[None, :]
    half_order = matrix_order // 2
    rotated = jnp.concatenate([-weights[half_order:], weights[:half_order]], axis=0)
    beam_taps = jnp.concatenate([weights, rotated], axis=1).astype(jnp.bfloat16)
    return (weights.T, beam_taps)

def reference(snapshots, train_gates, guard_keep, beam_cells):
    blocks = jnp.arange(TRAIN, dtype=jnp.int32) // TRAIN_DEV * GATES_DEV
    beam_list = []
    weight_list = []
    for bin_group in range(NB):
        gate_index = (blocks + train_gates[bin_group]).astype(jnp.int32)
        picked = jnp.take(snapshots[bin_group], gate_index, axis=1)
        picked = picked * guard_keep[bin_group][None, :, None].astype(jnp.bfloat16)
        direct = jnp.concatenate([picked[0], picked[1]], axis=1)
        turned = jnp.concatenate([-picked[1], picked[0]], axis=1)
        covariance = gram_product(direct, direct) + gram_product(turned, turned)
        weights, beam_taps = adapt(covariance, steering(beam_cells[bin_group]))
        weight_list.append(weights)
        composite = jnp.concatenate([snapshots[bin_group, 0], snapshots[bin_group, 1]], axis=1)
        outputs = lax.dot_general(beam_taps.astype(jnp.float32), composite.astype(jnp.float32), (((0,), (1,)), ((), ())), preferred_element_type=jnp.float32)
        beam_list.append(outputs.reshape(2, BEAMS, GATES).astype(jnp.bfloat16))
    return (jnp.stack(beam_list), jnp.stack(weight_list))
```

```python
import functools
import math

import jax
import jax.numpy as jnp
from jax import lax
from jax.experimental import pallas as pl
from jax.experimental.pallas import tpu as pltpu
from jax.sharding import PartitionSpec as P

ELEM = 16
PULSE = 12
ANGLES = 64
LOADING = 0.05
LANES = 128
STEPS = 8
REFINE = 2

MESH = pl.DeviceIdType.MESH
F32 = jnp.float32
BF16 = jnp.bfloat16


def dot_nn(left, right):
    return lax.dot_general(left, right, (((1,), (0,)), ((), ())), preferred_element_type=F32)


def dot_nt(left, right):
    return lax.dot_general(left, right, (((1,), (1,)), ((), ())), preferred_element_type=F32)


def dot_tn(left, right):
    return lax.dot_general(left, right, (((0,), (0,)), ((), ())), preferred_element_type=F32)


def halves(value):
    high = value.astype(BF16)
    return high, (value - high.astype(F32)).astype(BF16)


def exact_dot(dot, value, right):
    rows = value.shape[0]
    high, rest = halves(value)
    middle = (value - high.astype(F32)).astype(BF16)
    low = (value - high.astype(F32) - middle.astype(F32)).astype(BF16)
    product = dot(jnp.concatenate([high, middle, low], axis=0), right)
    return product[:rows] + (product[rows : 2 * rows] + product[2 * rows :])


def turn(value, pad):
    pieces = []
    for base in range(0, value.shape[1], 2 * pad):
        pieces += [-value[:, base + pad : base + 2 * pad], value[:, base : base + pad]]
    return jnp.concatenate(pieces, axis=1)


def steer_rows(cells, beams, chans, width, pad):
    cell = jnp.zeros((beams, pad), F32)
    row = lax.broadcasted_iota(jnp.int32, (beams, pad), 0)
    for k in range(beams):
        cell = jnp.where(row == k, cells(k).astype(F32), cell)
    angle = jnp.floor((cell + 0.5) * (1.0 / PULSE))
    doppler = cell - PULSE * angle
    lane = lax.broadcasted_iota(jnp.int32, (beams, pad), 1)
    whole = 2.0 * ANGLES * PULSE / 4.0
    blocks = []
    for c in range(chans):
        channel = (lane + c * width).astype(F32)
        pulse = jnp.floor((channel + 0.5) * (1.0 / ELEM))
        element = channel - ELEM * pulse
        count = (PULSE / 4.0) * element * (2.0 * angle + 1.0 - ANGLES) + (ANGLES / 4.0) * pulse * (
            2.0 * doppler + 1.0 - PULSE
        )
        count = count - whole * jnp.floor(count * (1.0 / whole) + 0.5)
        phase = count * (2.0 * math.pi / whole)
        norm_scale = jnp.where(lane < width, 1.0 / math.sqrt(chans * width), 0.0)
        blocks += [jnp.cos(phase) * norm_scale, jnp.sin(phase) * norm_scale]
    return jnp.concatenate(blocks, axis=1)


def solve_rows(direct, steer, order, pad, store):
    train = direct.shape[0]
    dual = 2 * train <= direct.shape[1]
    both = jnp.concatenate([direct, turn(direct, pad)], axis=0)
    squares = direct.astype(F32)
    trace = 2.0 * jnp.sum(jnp.sum(squares * squares, axis=0, keepdims=True), axis=1, keepdims=True)
    loading = LOADING * trace / order + 1e-06
    span = 0.5 * trace * (1.0 + 1e-05) + 1e-06
    if dual:
        top = dot_nt(direct, both)

        def expand(rows):
            left, right = rows[:, :train], rows[:, train:]
            return jnp.concatenate([rows, jnp.concatenate([-right, left], axis=1)], axis=0)

    else:
        top = dot_tn(both, both)

        def expand(rows):
            return rows

    height, size = top.shape
    eye = jnp.where(
        lax.broadcasted_iota(jnp.int32, (height, size), 0)
        == lax.broadcasted_iota(jnp.int32, (height, size), 1),
        1.0,
        0.0,
    ).astype(F32)
    ratio = span / (span + 2.0 * loading)
    gap = top * (2.0 / span)

    def factors(ratio):
        scale = 2.0 / (2.0 - ratio * ratio)
        return scale * (1.0 + ratio), scale * ratio, ratio * ratio / (2.0 - ratio * ratio)

    def pair(high, low):
        high, low = expand(high), expand(low)
        return jnp.concatenate([high, low, high], axis=0)

    keep, drop, ratio = factors(ratio)
    start = 2.0 / (2.0 * loading + span)
    inverse = start * (keep * eye - drop * gap)
    high, low = halves(gap)
    square = dot_nn(jnp.concatenate([high, high, low], axis=1), pair(high, low))
    gap = 4.0 * gap - 2.0 * square

    def step(carry):
        gap, inverse, ratio = carry
        keep, drop, ratio = factors(ratio)
        high, low = halves(gap)
        inv_high, inv_low = halves(inverse)
        left = jnp.concatenate(
            [
                jnp.concatenate([high, high, low], axis=1),
                jnp.concatenate([inv_high, inv_high, inv_low], axis=1),
            ],
            axis=0,
        )
        product = dot_nn(left, pair(high, low))
        return (
            4.0 * gap - 2.0 * product[:height],
            keep * inverse - drop * product[height:],
            ratio,
        )

    carry = (gap, inverse, ratio)
    if dual:
        for _ in range(STEPS - 1):
            carry = step(carry)
    else:
        gap_store, inverse_store = store
        gap_store[...] = gap
        inverse_store[...] = inverse

        def body(_, ratio):
            new_gap, new_inverse, new_ratio = step((gap_store[...], inverse_store[...], ratio))
            gap_store[...] = new_gap
            inverse_store[...] = new_inverse
            return new_ratio

        ratio = lax.fori_loop(0, STEPS - 1, body, ratio)
        carry = (None, inverse_store[...], ratio)
    stacked = pair(*halves(carry[1]))

    def precondition(value):
        high, low = halves(value)
        return dot_nn(jnp.concatenate([high, high, low], axis=1), stacked)

    if dual:
        right = exact_dot(dot_nt, steer, both)
    else:
        right = steer
    answer = precondition(right)
    for _ in range(REFINE):
        if dual:
            image = exact_dot(dot_nt, exact_dot(dot_nn, answer, both), both)
        else:
            image = exact_dot(dot_nn, exact_dot(dot_nt, answer, both), both)
        answer = answer + precondition(right - loading * answer - image)
    if dual:
        answer = steer - exact_dot(dot_nn, answer, both)
    gain = jnp.sum(steer * answer, axis=1, keepdims=True)
    return answer / gain


def kernel(
    rng_count,
    chans,
    pad,
    snap,
    gates,
    guard,
    cells,
    out,
    weights_out,
    full,
    cube,
    piece,
    rows,
    taps_store,
    *rest,
):
    store, sems = rest[:-9], rest[-9:]
    full_sem, own_sem, half_send, half_recv, row_send, row_recv, row_own, tap_send, tap_recv = sems
    groups, _, width, span = snap.shape
    beams = weights_out.shape[1]
    train_dev = gates.shape[1]
    half = span // chans
    place = lax.axis_index("rng")
    chan = lax.axis_index("chan")
    mine = lax.rem(place, groups)
    cluster = place - mine

    loads = []
    for g in range(groups):
        load = pltpu.make_async_copy(snap.at[g], full.at[g], full_sem.at[g])
        load.start()
        loads.append(load)

    barrier = pltpu.get_barrier_semaphore()
    for d in range(rng_count):
        for e in range(chans):
            if d == 0 and e == 0:
                continue
            pl.semaphore_signal(
                barrier,
                inc=1,
                device_id={
                    "rng": lax.rem(place + d, rng_count),
                    "chan": lax.rem(chan + e, chans),
                },
                device_id_type=MESH,
            )

    own_start = pl.multiple_of(chan * half, LANES)
    owns = []
    for g in range(groups):
        own = pltpu.make_async_copy(
            snap.at[g, :, :, pl.ds(own_start, half)],
            cube.at[g, chan, :, pl.ds(0, width), :],
            own_sem.at[g],
        )
        own.start()
        owns.append(own)
    if pad > width:
        for g in range(groups):
            for c in range(chans):
                for q in range(2):
                    cube[g, c, q, pl.ds(width, pad - width), :] = jnp.zeros(
                        (pad - width, half), BF16
                    )
    piece[...] = jnp.zeros_like(piece)
    steer = steer_rows(lambda k: cells[mine, k], beams, chans, width, pad)

    row = lax.broadcasted_iota(jnp.int32, (train_dev, LANES), 0)
    lane = lax.broadcasted_iota(jnp.int32, (train_dev, LANES), 1)
    for g in range(groups):
        chosen = jnp.full((train_dev, LANES), -1, jnp.int32)
        for t in range(train_dev):
            chosen = jnp.where(
                row == t, jnp.where(guard[g, t] != 0, gates[g, t], -1), chosen
            )
        offset = chosen - lane
        onehot = jnp.concatenate(
            [
                jnp.where(offset == base, 1.0, 0.0).astype(BF16)
                for base in range(0, span, LANES)
            ],
            axis=1,
        )
        loads[g].wait()
        for q in range(2):
            piece[g, :, pl.ds(q * pad, width)] = dot_nt(onehot, full[g, q]).astype(BF16)

    pl.semaphore_wait(barrier, rng_count * chans - 1)

    row_copies = []
    for d in range(rng_count - 1, -1, -1):
        target = lax.rem(place + d, rng_count)
        for e in range(chans):
            if d == 0 and e == 0:
                continue
            copy = pltpu.make_async_remote_copy(
                src_ref=piece.at[lax.rem(target, groups)],
                dst_ref=rows.at[place, chan],
                send_sem=row_send.at[d, e],
                recv_sem=row_recv.at[place, chan],
                device_id={"rng": target, "chan": lax.rem(chan + e, chans)},
                device_id_type=MESH,
            )
            copy.start()
            row_copies.append(copy)
    own_rows = pltpu.make_async_copy(piece.at[mine], rows.at[place, chan], row_own)
    own_rows.start()

    half_copies = []
    for g in range(groups):
        for e in range(1, chans):
            other = lax.rem(chan + e, chans)
            copy = pltpu.make_async_remote_copy(
                src_ref=snap.at[g, :, :, pl.ds(pl.multiple_of(other * half, LANES), half)],
                dst_ref=cube.at[g, chan, :, pl.ds(0, width), :],
                send_sem=half_send.at[g, e],
                recv_sem=half_recv.at[g, e],
                device_id={"chan": other},
                device_id_type=MESH,
            )
            copy.start()
            half_copies.append(copy)

    own_rows.wait()
    for d in range(rng_count):
        source = lax.rem(place + d, rng_count)
        for e in range(chans):
            if d == 0 and e == 0:
                continue
            from_chan = lax.rem(chan + e, chans)
            pltpu.make_async_copy(
                rows.at[source, from_chan],
                rows.at[source, from_chan],
                row_recv.at[source, from_chan],
            ).wait()

    direct = jnp.concatenate(
        [rows[:, c].reshape(rng_count * train_dev, 2 * pad) for c in range(chans)], axis=1
    )
    taps_store[mine] = solve_rows(direct, steer, 2 * chans * width, pad, store)

    tap_copies = []
    for d in range(1, groups):
        copy = pltpu.make_async_remote_copy(
            src_ref=taps_store.at[mine],
            dst_ref=taps_store.at[mine],
            send_sem=tap_send.at[d],
            recv_sem=tap_recv.at[mine],
            device_id={"rng": cluster + lax.rem(mine + d, groups)},
            device_id_type=MESH,
        )
        copy.start()
        tap_copies.append(copy)

    for own in owns:
        own.wait()
    for copy in half_copies:
        copy.wait()
    for d in range(groups):
        g = lax.rem(mine + d, groups)
        if d > 0:
            pltpu.make_async_copy(taps_store.at[g], taps_store.at[g], tap_recv.at[g]).wait()
        weights = taps_store[g]
        taps = jnp.concatenate([weights, turn(weights, pad)], axis=0).astype(BF16)
        samples = cube[g].reshape(chans * 2 * pad, half)
        out[g] = dot_nn(taps, samples).astype(BF16).reshape(2, beams, half)
        weights_out[g] = jnp.concatenate(
            [
                weights[:, c * 2 * pad + q * pad : c * 2 * pad + q * pad + width]
                for q in range(2)
                for c in range(chans)
            ],
            axis=1,
        )
    for copy in row_copies:
        copy.wait_send()
    for copy in tap_copies:
        copy.wait_send()


def per_device(rng_count, chans, snapshots, train_gates, guard_keep, beam_cells):
    groups, _, span, width = snapshots.shape
    beams = beam_cells.shape[1]
    train_dev = train_gates.shape[1]
    pad = -(-width // LANES) * LANES
    half = span // chans
    lanes = chans * 2 * pad
    store = []
    if 2 * rng_count * train_dev > lanes:
        store = [pltpu.VMEM((lanes, lanes), F32), pltpu.VMEM((lanes, lanes), F32)]
    dma = pltpu.SemaphoreType.DMA
    return pl.pallas_call(
        functools.partial(kernel, rng_count, chans, pad),
        out_shape=(
            jax.ShapeDtypeStruct((groups, 2, beams, half), BF16),
            jax.ShapeDtypeStruct((groups, beams, chans * 2 * width), F32),
        ),
        in_specs=[
            pl.BlockSpec(memory_space=pl.ANY),
            pl.BlockSpec(memory_space=pltpu.SMEM),
            pl.BlockSpec(memory_space=pltpu.SMEM),
            pl.BlockSpec(memory_space=pltpu.SMEM),
        ],
        out_specs=(
            pl.BlockSpec(memory_space=pltpu.VMEM),
            pl.BlockSpec(memory_space=pltpu.VMEM),
        ),
        scratch_shapes=[
            pltpu.VMEM((groups, 2, width, span), BF16),
            pltpu.VMEM((groups, chans, 2, pad, half), BF16),
            pltpu.VMEM((groups, train_dev, 2 * pad), BF16),
            pltpu.VMEM((rng_count, chans, train_dev, 2 * pad), BF16),
            pltpu.VMEM((groups, beams, lanes), F32),
            *store,
            dma((groups,)),
            dma((groups,)),
            dma((groups, chans)),
            dma((groups, chans)),
            dma((rng_count, chans)),
            dma((rng_count, chans)),
            dma,
            dma((groups,)),
            dma((groups,)),
        ],
        compiler_params=pltpu.CompilerParams(
            collective_id=0, has_side_effects=True, vmem_limit_bytes=56 * 1024 * 1024
        ),
    )(jnp.transpose(snapshots, (0, 1, 3, 2)), train_gates, guard_keep, beam_cells)


def solution(mesh):
    placed = (
        P("parts", None, "rng", "chan"),
        P("parts", "rng"),
        P("parts", "rng"),
        P("parts", None),
    )
    return jax.shard_map(
        functools.partial(per_device, mesh.shape["rng"], mesh.shape["chan"]),
        mesh=mesh,
        in_specs=placed,
        out_specs=(P("parts", None, None, ("rng", "chan")), P("parts", None, None)),
        check_vma=False,
    )
```

```python
import functools
import math

import jax
import jax.numpy as jnp
from jax import lax
from jax.experimental import pallas as pl
from jax.experimental.pallas import tpu as pltpu
from jax.sharding import PartitionSpec as P

ELEM = 16
PULSE = 12
ANGLES = 64
LOADING = 0.05
LANES = 128
STEPS = 8
REFINE = 3

MESH = pl.DeviceIdType.MESH
F32 = jnp.float32
BF16 = jnp.bfloat16


def dot_nn(left, right):
    return lax.dot_general(left, right, (((1,), (0,)), ((), ())), preferred_element_type=F32)


def dot_nt(left, right):
    return lax.dot_general(left, right, (((1,), (1,)), ((), ())), preferred_element_type=F32)


def dot_tn(left, right):
    return lax.dot_general(left, right, (((0,), (0,)), ((), ())), preferred_element_type=F32)


def halves(value):
    high = value.astype(BF16)
    return high, (value - high.astype(F32)).astype(BF16)


def exact_dot(dot, value, right):
    rows = value.shape[0]
    high, rest = halves(value)
    middle = (value - high.astype(F32)).astype(BF16)
    low = (value - high.astype(F32) - middle.astype(F32)).astype(BF16)
    product = dot(jnp.concatenate([high, middle, low], axis=0), right)
    return product[:rows] + (product[rows : 2 * rows] + product[2 * rows :])


def turn(value, pad):
    pieces = []
    for base in range(0, value.shape[1], 2 * pad):
        pieces += [-value[:, base + pad : base + 2 * pad], value[:, base : base + pad]]
    return jnp.concatenate(pieces, axis=1)


def steer_rows(cells, beams, chans, width, pad):
    cell = jnp.zeros((beams, pad), F32)
    row = lax.broadcasted_iota(jnp.int32, (beams, pad), 0)
    for k in range(beams):
        cell = jnp.where(row == k, cells(k).astype(F32), cell)
    angle = jnp.floor((cell + 0.5) * (1.0 / PULSE))
    doppler = cell - PULSE * angle
    lane = lax.broadcasted_iota(jnp.int32, (beams, pad), 1)
    whole = 2.0 * ANGLES * PULSE / 4.0
    blocks = []
    for c in range(chans):
        channel = (lane + c * width).astype(F32)
        pulse = jnp.floor((channel + 0.5) * (1.0 / ELEM))
        element = channel - ELEM * pulse
        count = (PULSE / 4.0) * element * (2.0 * angle + 1.0 - ANGLES) + (ANGLES / 4.0) * pulse * (
            2.0 * doppler + 1.0 - PULSE
        )
        count = count - whole * jnp.floor(count * (1.0 / whole) + 0.5)
        phase = count * (2.0 * math.pi / whole)
        norm_scale = jnp.where(lane < width, 1.0 / math.sqrt(chans * width), 0.0)
        blocks += [jnp.cos(phase) * norm_scale, jnp.sin(phase) * norm_scale]
    return jnp.concatenate(blocks, axis=1)


def solve_rows(direct, steer, order, pad, store):
    train = direct.shape[0]
    dual = 2 * train <= direct.shape[1]
    both = jnp.concatenate([direct, turn(direct, pad)], axis=0)
    squares = direct.astype(F32)
    trace = 2.0 * jnp.sum(jnp.sum(squares * squares, axis=0, keepdims=True), axis=1, keepdims=True)
    loading = LOADING * trace / order + 1e-06
    span = 0.5 * trace * (1.0 + 1e-05) + 1e-06
    if dual:
        top = dot_nt(direct, both)

        def expand(rows):
            left, right = rows[:, :train], rows[:, train:]
            return jnp.concatenate([rows, jnp.concatenate([-right, left], axis=1)], axis=0)

    else:
        top = dot_tn(both, both)

        def expand(rows):
            return rows

    height, size = top.shape
    eye = jnp.where(
        lax.broadcasted_iota(jnp.int32, (height, size), 0)
        == lax.broadcasted_iota(jnp.int32, (height, size), 1),
        1.0,
        0.0,
    ).astype(F32)
    ratio = span / (span + 2.0 * loading)
    gap = top * (2.0 / span)

    def factors(ratio):
        scale = 2.0 / (2.0 - ratio * ratio)
        return scale * (1.0 + ratio), scale * ratio, ratio * ratio / (2.0 - ratio * ratio)

    def pair(high, low):
        high, low = expand(high), expand(low)
        return jnp.concatenate([high, low, high], axis=0)

    keep, drop, ratio = factors(ratio)
    start = 2.0 / (2.0 * loading + span)
    inverse = start * (keep * eye - drop * gap)
    high, low = halves(gap)
    square = dot_nn(jnp.concatenate([high, high, low], axis=1), pair(high, low))
    gap = 4.0 * gap - 2.0 * square

    def step(carry):
        gap, inverse, ratio = carry
        keep, drop, ratio = factors(ratio)
        high, low = halves(gap)
        inv_high, inv_low = halves(inverse)
        left = jnp.concatenate(
            [
                jnp.concatenate([high, high, low], axis=1),
                jnp.concatenate([inv_high, inv_high, inv_low], axis=1),
            ],
            axis=0,
        )
        product = dot_nn(left, pair(high, low))
        return (
            4.0 * gap - 2.0 * product[:height],
            keep * inverse - drop * product[height:],
            ratio,
        )

    carry = (gap, inverse, ratio)
    if dual:
        for _ in range(STEPS - 1):
            carry = step(carry)
    else:
        gap_store, inverse_store = store
        gap_store[...] = gap
        inverse_store[...] = inverse

        def body(_, ratio):
            new_gap, new_inverse, new_ratio = step((gap_store[...], inverse_store[...], ratio))
            gap_store[...] = new_gap
            inverse_store[...] = new_inverse
            return new_ratio

        ratio = lax.fori_loop(0, STEPS - 1, body, ratio)
        carry = (None, inverse_store[...], ratio)
    stacked = pair(*halves(carry[1]))

    def precondition(value):
        high, low = halves(value)
        return dot_nn(jnp.concatenate([high, high, low], axis=1), stacked)

    if dual:
        right = exact_dot(dot_nt, steer, both)
    else:
        right = steer
    answer = precondition(right)
    for _ in range(REFINE):
        if dual:
            image = exact_dot(dot_nt, exact_dot(dot_nn, answer, both), both)
        else:
            image = exact_dot(dot_nn, exact_dot(dot_nt, answer, both), both)
        answer = answer + precondition(right - loading * answer - image)
    if dual:
        answer = steer - exact_dot(dot_nn, answer, both)
    gain = jnp.sum(steer * answer, axis=1, keepdims=True)
    return answer / gain


def kernel(
    rng_count,
    chans,
    pad,
    snap,
    gates,
    guard,
    cells,
    out,
    weights_out,
    full,
    cube,
    piece,
    rows,
    *rest,
):
    store, sems = rest[:-9], rest[-9:]
    full_sem, own_sem, half_send, half_recv, row_send, row_recv, row_own, tap_send, tap_recv = sems
    groups, _, width, span = snap.shape
    beams = weights_out.shape[1]
    train_dev = gates.shape[1]
    half = span // chans
    place = lax.axis_index("rng")
    chan = lax.axis_index("chan")
    chips = groups // chans
    spot = lax.rem(place, chips)
    mine = spot * chans + chan
    cluster = place - spot

    loads = []
    for g in range(groups):
        load = pltpu.make_async_copy(snap.at[g], full.at[g], full_sem.at[g])
        load.start()
        loads.append(load)

    barrier = pltpu.get_barrier_semaphore()
    for d in range(rng_count):
        for e in range(chans):
            if d == 0 and e == 0:
                continue
            pl.semaphore_signal(
                barrier,
                inc=1,
                device_id={
                    "rng": lax.rem(place + d, rng_count),
                    "chan": lax.rem(chan + e, chans),
                },
                device_id_type=MESH,
            )

    own_start = pl.multiple_of(chan * half, LANES)
    owns = []
    for g in range(groups):
        own = pltpu.make_async_copy(
            snap.at[g, :, :, pl.ds(own_start, half)],
            cube.at[g, :, chan],
            own_sem.at[g],
        )
        own.start()
        owns.append(own)
    piece[...] = jnp.zeros_like(piece)
    steer = steer_rows(lambda k: cells[mine, k], beams, chans, width, pad)

    row = lax.broadcasted_iota(jnp.int32, (train_dev, LANES), 0)
    lane = lax.broadcasted_iota(jnp.int32, (train_dev, LANES), 1)
    for g in range(groups):
        chosen = jnp.full((train_dev, LANES), -1, jnp.int32)
        for t in range(train_dev):
            chosen = jnp.where(
                row == t, jnp.where(guard[g, t] != 0, gates[g, t], -1), chosen
            )
        offset = chosen - lane
        onehot = jnp.concatenate(
            [
                jnp.where(offset == base, 1.0, 0.0).astype(BF16)
                for base in range(0, span, LANES)
            ],
            axis=1,
        )
        loads[g].wait()
        for q in range(2):
            piece[g, :, pl.ds(q * pad, width)] = dot_nt(onehot, full[g, q]).astype(BF16)

    pl.semaphore_wait(barrier, rng_count * chans - 1)

    row_copies = []
    for d in range(rng_count - 1, -1, -1):
        target = lax.rem(place + d, rng_count)
        for e in range(chans):
            if d == 0 and e == 0:
                continue
            to_chan = lax.rem(chan + e, chans)
            copy = pltpu.make_async_remote_copy(
                src_ref=piece.at[lax.rem(target, chips) * chans + to_chan],
                dst_ref=rows.at[place, chan],
                send_sem=row_send.at[d, e],
                recv_sem=row_recv.at[place, chan],
                device_id={"rng": target, "chan": to_chan},
                device_id_type=MESH,
            )
            copy.start()
            row_copies.append(copy)
    own_rows = pltpu.make_async_copy(piece.at[mine], rows.at[place, chan], row_own)
    own_rows.start()

    half_copies = []
    for g in range(groups):
        for e in range(1, chans):
            other = lax.rem(chan + e, chans)
            copy = pltpu.make_async_remote_copy(
                src_ref=snap.at[g, :, :, pl.ds(pl.multiple_of(other * half, LANES), half)],
                dst_ref=cube.at[g, :, chan],
                send_sem=half_send.at[g, e],
                recv_sem=half_recv.at[g, e],
                device_id={"chan": other},
                device_id_type=MESH,
            )
            copy.start()
            half_copies.append(copy)

    own_rows.wait()
    for d in range(rng_count):
        source = lax.rem(place + d, rng_count)
        for e in range(chans):
            if d == 0 and e == 0:
                continue
            from_chan = lax.rem(chan + e, chans)
            pltpu.make_async_copy(
                rows.at[source, from_chan],
                rows.at[source, from_chan],
                row_recv.at[source, from_chan],
            ).wait()

    direct = jnp.concatenate(
        [rows[:, c].reshape(rng_count * train_dev, 2 * pad) for c in range(chans)], axis=1
    )
    weights = solve_rows(direct, steer, 2 * chans * width, pad, store)
    weights_out[mine] = jnp.concatenate(
        [
            weights[:, c * 2 * pad + q * pad : c * 2 * pad + q * pad + width]
            for q in range(2)
            for c in range(chans)
        ],
        axis=1,
    )

    tap_copies = []
    for d in range(chips - 1, -1, -1):
        for e in range(chans):
            if d == 0 and e == 0:
                continue
            copy = pltpu.make_async_remote_copy(
                src_ref=weights_out.at[mine],
                dst_ref=weights_out.at[mine],
                send_sem=tap_send.at[d, e],
                recv_sem=tap_recv.at[mine],
                device_id={
                    "rng": cluster + lax.rem(spot + d, chips),
                    "chan": lax.rem(chan + e, chans),
                },
                device_id_type=MESH,
            )
            copy.start()
            tap_copies.append(copy)

    for own in owns:
        own.wait()
    for copy in half_copies:
        copy.wait()
    for d in range(chips):
        for e in range(chans):
            g = lax.rem(spot + d, chips) * chans + lax.rem(chan + e, chans)
            if d > 0 or e > 0:
                pltpu.make_async_copy(
                    weights_out.at[g], weights_out.at[g], tap_recv.at[g]
                ).wait()
            weights = weights_out[g]
            turned = jnp.concatenate(
                [-weights[:, chans * width :], weights[:, : chans * width]], axis=1
            )
            taps = jnp.concatenate([weights, turned], axis=0).astype(BF16)
            samples = cube[g].reshape(2 * chans * width, half)
            out[g] = dot_nn(taps, samples).astype(BF16).reshape(2, beams, half)
    for copy in row_copies:
        copy.wait_send()
    for copy in tap_copies:
        copy.wait_send()


def per_device(rng_count, chans, snapshots, train_gates, guard_keep, beam_cells):
    groups, _, span, width = snapshots.shape
    beams = beam_cells.shape[1]
    train_dev = train_gates.shape[1]
    pad = -(-width // LANES) * LANES
    half = span // chans
    lanes = chans * 2 * pad
    store = []
    if 2 * rng_count * train_dev > lanes:
        store = [pltpu.VMEM((lanes, lanes), F32), pltpu.VMEM((lanes, lanes), F32)]
    dma = pltpu.SemaphoreType.DMA
    results = pl.pallas_call(
        functools.partial(kernel, rng_count, chans, pad),
        out_shape=(
            pltpu.VMEM((groups, 2, beams, half), BF16),
            pltpu.VMEM((groups, beams, chans * 2 * width), F32),
        ),
        in_specs=[
            pl.BlockSpec(memory_space=pl.ANY),
            pl.BlockSpec(memory_space=pltpu.SMEM),
            pl.BlockSpec(memory_space=pltpu.SMEM),
            pl.BlockSpec(memory_space=pltpu.SMEM),
        ],
        out_specs=(
            pl.BlockSpec(memory_space=pltpu.VMEM),
            pl.BlockSpec(memory_space=pltpu.VMEM),
        ),
        scratch_shapes=[
            pltpu.VMEM((groups, 2, width, span), BF16),
            pltpu.VMEM((groups, 2, chans, width, half), BF16),
            pltpu.VMEM((groups, train_dev, 2 * pad), BF16),
            pltpu.VMEM((rng_count, chans, train_dev, 2 * pad), BF16),
            *store,
            dma((groups,)),
            dma((groups,)),
            dma((groups, chans)),
            dma((groups, chans)),
            dma((rng_count, chans)),
            dma((rng_count, chans)),
            dma,
            dma((groups // chans, chans)),
            dma((groups,)),
        ],
        compiler_params=pltpu.CompilerParams(
            collective_id=0, has_side_effects=True, vmem_limit_bytes=56 * 1024 * 1024
        ),
    )(jnp.transpose(snapshots, (0, 1, 3, 2)), train_gates, guard_keep, beam_cells)
    return pl.pallas_call(
        write_out,
        out_shape=tuple(jax.ShapeDtypeStruct(r.shape, r.dtype) for r in results),
        in_specs=[pl.BlockSpec(memory_space=pltpu.VMEM)] * 2,
        out_specs=(pl.BlockSpec(memory_space=pl.ANY), pl.BlockSpec(memory_space=pl.ANY)),
        scratch_shapes=[dma((2,))],
        compiler_params=pltpu.CompilerParams(vmem_limit_bytes=4 * 1024 * 1024),
    )(*results)


def write_out(beams_in, weights_in, beams_out, weights_out, sem):
    copies = [
        pltpu.make_async_copy(beams_in, beams_out, sem.at[0]),
        pltpu.make_async_copy(weights_in, weights_out, sem.at[1]),
    ]
    for copy in copies:
        copy.start()
    for copy in copies:
        copy.wait()


def solution(mesh):
    placed = (
        P("parts", None, "rng", "chan"),
        P("parts", "rng"),
        P("parts", "rng"),
        P("parts", None),
    )
    return jax.shard_map(
        functools.partial(per_device, mesh.shape["rng"], mesh.shape["chan"]),
        mesh=mesh,
        in_specs=placed,
        out_specs=(P("parts", None, None, ("rng", "chan")), P("parts", None, None)),
        check_vma=False,
    )
```

```python
import functools
import math

import jax
import jax.numpy as jnp
from jax import lax
from jax.experimental import pallas as pl
from jax.experimental.pallas import tpu as pltpu
from jax.sharding import PartitionSpec as P

ELEM = 16
PULSE = 12
ANGLES = 64
LOADING = 0.05
LANES = 128
STEPS = 8
REFINE = 3

MESH = pl.DeviceIdType.MESH
F32 = jnp.float32
BF16 = jnp.bfloat16


def dot_nn(left, right):
    return lax.dot_general(left, right, (((1,), (0,)), ((), ())), preferred_element_type=F32)


def dot_nt(left, right):
    return lax.dot_general(left, right, (((1,), (1,)), ((), ())), preferred_element_type=F32)


def dot_tn(left, right):
    return lax.dot_general(left, right, (((0,), (0,)), ((), ())), preferred_element_type=F32)


def halves(value):
    high = value.astype(BF16)
    return high, (value - high.astype(F32)).astype(BF16)


def exact_dot(dot, value, right):
    rows = value.shape[0]
    high, rest = halves(value)
    middle = (value - high.astype(F32)).astype(BF16)
    low = (value - high.astype(F32) - middle.astype(F32)).astype(BF16)
    product = dot(jnp.concatenate([high, middle, low], axis=0), right)
    return product[:rows] + (product[rows : 2 * rows] + product[2 * rows :])


def turn(value, pad):
    pieces = []
    for base in range(0, value.shape[1], 2 * pad):
        pieces += [-value[:, base + pad : base + 2 * pad], value[:, base : base + pad]]
    return jnp.concatenate(pieces, axis=1)


def steer_rows(cells, beams, chans, width, pad):
    cell = jnp.zeros((beams, pad), F32)
    row = lax.broadcasted_iota(jnp.int32, (beams, pad), 0)
    for k in range(beams):
        cell = jnp.where(row == k, cells(k).astype(F32), cell)
    angle = jnp.floor((cell + 0.5) * (1.0 / PULSE))
    doppler = cell - PULSE * angle
    lane = lax.broadcasted_iota(jnp.int32, (beams, pad), 1)
    whole = 2.0 * ANGLES * PULSE / 4.0
    blocks = []
    for c in range(chans):
        channel = (lane + c * width).astype(F32)
        pulse = jnp.floor((channel + 0.5) * (1.0 / ELEM))
        element = channel - ELEM * pulse
        count = (PULSE / 4.0) * element * (2.0 * angle + 1.0 - ANGLES) + (ANGLES / 4.0) * pulse * (
            2.0 * doppler + 1.0 - PULSE
        )
        count = count - whole * jnp.floor(count * (1.0 / whole) + 0.5)
        phase = count * (2.0 * math.pi / whole)
        norm_scale = jnp.where(lane < width, 1.0 / math.sqrt(chans * width), 0.0)
        blocks += [jnp.cos(phase) * norm_scale, jnp.sin(phase) * norm_scale]
    return jnp.concatenate(blocks, axis=1)


def solve_rows(direct, steer, order, pad, store):
    train = direct.shape[0]
    dual = 2 * train <= direct.shape[1]
    both = jnp.concatenate([direct, turn(direct, pad)], axis=0)
    squares = direct.astype(F32)
    trace = 2.0 * jnp.sum(jnp.sum(squares * squares, axis=0, keepdims=True), axis=1, keepdims=True)
    loading = LOADING * trace / order + 1e-06
    span = 0.5 * trace * (1.0 + 1e-05) + 1e-06
    if dual:
        top = dot_nt(direct, both)

        def expand(rows):
            left, right = rows[:, :train], rows[:, train:]
            return jnp.concatenate([rows, jnp.concatenate([-right, left], axis=1)], axis=0)

    else:
        top = dot_tn(both, both)

        def expand(rows):
            return rows

    height, size = top.shape
    eye = jnp.where(
        lax.broadcasted_iota(jnp.int32, (height, size), 0)
        == lax.broadcasted_iota(jnp.int32, (height, size), 1),
        1.0,
        0.0,
    ).astype(F32)
    ratio = span / (span + 2.0 * loading)
    gap = top * (2.0 / span)

    def factors(ratio):
        scale = 2.0 / (2.0 - ratio * ratio)
        return scale * (1.0 + ratio), scale * ratio, ratio * ratio / (2.0 - ratio * ratio)

    def pair(high, low):
        high, low = expand(high), expand(low)
        return jnp.concatenate([high, low, high], axis=0)

    keep, drop, ratio = factors(ratio)
    start = 2.0 / (2.0 * loading + span)
    inverse = start * (keep * eye - drop * gap)
    high, low = halves(gap)
    square = dot_nn(jnp.concatenate([high, high, low], axis=1), pair(high, low))
    gap = 4.0 * gap - 2.0 * square

    def step(carry):
        gap, inverse, ratio = carry
        keep, drop, ratio = factors(ratio)
        high, low = halves(gap)
        inv_high, inv_low = halves(inverse)
        left = jnp.concatenate(
            [
                jnp.concatenate([high, high, low], axis=1),
                jnp.concatenate([inv_high, inv_high, inv_low], axis=1),
            ],
            axis=0,
        )
        product = dot_nn(left, pair(high, low))
        return (
            4.0 * gap - 2.0 * product[:height],
            keep * inverse - drop * product[height:],
            ratio,
        )

    carry = (gap, inverse, ratio)
    if dual:
        for _ in range(STEPS - 1):
            carry = step(carry)
    else:
        gap_store, inverse_store = store
        gap_store[...] = gap
        inverse_store[...] = inverse

        def body(_, ratio):
            new_gap, new_inverse, new_ratio = step((gap_store[...], inverse_store[...], ratio))
            gap_store[...] = new_gap
            inverse_store[...] = new_inverse
            return new_ratio

        ratio = lax.fori_loop(0, STEPS - 1, body, ratio)
        carry = (None, inverse_store[...], ratio)
    stacked = pair(*halves(carry[1]))

    def precondition(value):
        high, low = halves(value)
        return dot_nn(jnp.concatenate([high, high, low], axis=1), stacked)

    if dual:
        right = exact_dot(dot_nt, steer, both)
    else:
        right = steer
    answer = precondition(right)
    for _ in range(REFINE):
        if dual:
            image = exact_dot(dot_nt, exact_dot(dot_nn, answer, both), both)
        else:
            image = exact_dot(dot_nn, exact_dot(dot_nt, answer, both), both)
        answer = answer + precondition(right - loading * answer - image)
    if dual:
        answer = steer - exact_dot(dot_nn, answer, both)
    gain = jnp.sum(steer * answer, axis=1, keepdims=True)
    return answer / gain


def kernel(
    rng_count,
    chans,
    pad,
    snap,
    gates_in,
    guard_in,
    cells_in,
    out,
    weights_out,
    full,
    cube,
    piece,
    rows,
    gates,
    guard,
    cells,
    scalar_sem,
    *rest,
):
    store, sems = rest[:-9], rest[-9:]
    full_sem, own_sem, half_send, half_recv, row_send, row_recv, row_own, tap_send, tap_recv = sems
    groups, _, width, span = snap.shape
    beams = weights_out.shape[1]
    train_dev = gates.shape[1]
    half = span // chans
    place = lax.axis_index("rng")
    chan = lax.axis_index("chan")
    chips = groups // chans
    spot = lax.rem(place, chips)
    mine = spot * chans + chan
    cluster = place - spot

    barrier = pltpu.get_barrier_semaphore()
    for d in range(rng_count):
        for e in range(chans):
            if d == 0 and e == 0:
                continue
            pl.semaphore_signal(
                barrier,
                inc=1,
                device_id={
                    "rng": lax.rem(place + d, rng_count),
                    "chan": lax.rem(chan + e, chans),
                },
                device_id_type=MESH,
            )

    scalars = [
        pltpu.make_async_copy(source, held, scalar_sem.at[n])
        for n, (source, held) in enumerate(
            ((gates_in, gates), (guard_in, guard), (cells_in, cells))
        )
    ]
    for scalar in scalars:
        scalar.start()
    loads = []
    for g in range(groups):
        load = pltpu.make_async_copy(snap.at[g], full.at[g], full_sem.at[g])
        load.start()
        loads.append(load)

    own_start = pl.multiple_of(chan * half, LANES)
    owns = []
    for g in range(groups):
        own = pltpu.make_async_copy(
            snap.at[g, :, :, pl.ds(own_start, half)],
            cube.at[g, :, chan],
            own_sem.at[g],
        )
        own.start()
        owns.append(own)
    piece[...] = jnp.zeros_like(piece)
    for scalar in scalars:
        scalar.wait()
    steer = steer_rows(lambda k: cells[mine, k], beams, chans, width, pad)

    row = lax.broadcasted_iota(jnp.int32, (train_dev, LANES), 0)
    lane = lax.broadcasted_iota(jnp.int32, (train_dev, LANES), 1)
    for g in range(groups):
        chosen = jnp.full((train_dev, LANES), -1, jnp.int32)
        for t in range(train_dev):
            chosen = jnp.where(
                row == t, jnp.where(guard[g, t] != 0, gates[g, t], -1), chosen
            )
        offset = chosen - lane
        onehot = jnp.concatenate(
            [
                jnp.where(offset == base, 1.0, 0.0).astype(BF16)
                for base in range(0, span, LANES)
            ],
            axis=1,
        )
        loads[g].wait()
        for q in range(2):
            piece[g, :, pl.ds(q * pad, width)] = dot_nt(onehot, full[g, q]).astype(BF16)

    pl.semaphore_wait(barrier, rng_count * chans - 1)

    row_copies = []
    for d in range(rng_count - 1, -1, -1):
        target = lax.rem(place + d, rng_count)
        for e in range(chans):
            if d == 0 and e == 0:
                continue
            to_chan = lax.rem(chan + e, chans)
            copy = pltpu.make_async_remote_copy(
                src_ref=piece.at[lax.rem(target, chips) * chans + to_chan],
                dst_ref=rows.at[place, chan],
                send_sem=row_send.at[d, e],
                recv_sem=row_recv.at[place, chan],
                device_id={"rng": target, "chan": to_chan},
                device_id_type=MESH,
            )
            copy.start()
            row_copies.append(copy)
    own_rows = pltpu.make_async_copy(piece.at[mine], rows.at[place, chan], row_own)
    own_rows.start()

    half_copies = []
    for g in range(groups):
        for e in range(1, chans):
            other = lax.rem(chan + e, chans)
            copy = pltpu.make_async_remote_copy(
                src_ref=snap.at[g, :, :, pl.ds(pl.multiple_of(other * half, LANES), half)],
                dst_ref=cube.at[g, :, chan],
                send_sem=half_send.at[g, e],
                recv_sem=half_recv.at[g, e],
                device_id={"chan": other},
                device_id_type=MESH,
            )
            copy.start()
            half_copies.append(copy)

    own_rows.wait()
    for d in range(rng_count):
        source = lax.rem(place + d, rng_count)
        for e in range(chans):
            if d == 0 and e == 0:
                continue
            from_chan = lax.rem(chan + e, chans)
            pltpu.make_async_copy(
                rows.at[source, from_chan],
                rows.at[source, from_chan],
                row_recv.at[source, from_chan],
            ).wait()

    direct = jnp.concatenate(
        [rows[:, c].reshape(rng_count * train_dev, 2 * pad) for c in range(chans)], axis=1
    )
    weights = solve_rows(direct, steer, 2 * chans * width, pad, store)
    weights_out[mine] = jnp.concatenate(
        [
            weights[:, c * 2 * pad + q * pad : c * 2 * pad + q * pad + width]
            for q in range(2)
            for c in range(chans)
        ],
        axis=1,
    )

    tap_copies = []
    for d in range(chips - 1, -1, -1):
        for e in range(chans):
            if d == 0 and e == 0:
                continue
            copy = pltpu.make_async_remote_copy(
                src_ref=weights_out.at[mine],
                dst_ref=weights_out.at[mine],
                send_sem=tap_send.at[d, e],
                recv_sem=tap_recv.at[mine],
                device_id={
                    "rng": cluster + lax.rem(spot + d, chips),
                    "chan": lax.rem(chan + e, chans),
                },
                device_id_type=MESH,
            )
            copy.start()
            tap_copies.append(copy)

    for own in owns:
        own.wait()
    for copy in half_copies:
        copy.wait()
    for d in range(chips):
        for e in range(chans):
            g = lax.rem(spot + d, chips) * chans + lax.rem(chan + e, chans)
            if d > 0 or e > 0:
                pltpu.make_async_copy(
                    weights_out.at[g], weights_out.at[g], tap_recv.at[g]
                ).wait()
            weights = weights_out[g]
            turned = jnp.concatenate(
                [-weights[:, chans * width :], weights[:, : chans * width]], axis=1
            )
            taps = jnp.concatenate([weights, turned], axis=0).astype(BF16)
            samples = cube[g].reshape(2 * chans * width, half)
            out[g] = dot_nn(taps, samples).astype(BF16).reshape(2, beams, half)
    for copy in row_copies:
        copy.wait_send()
    for copy in tap_copies:
        copy.wait_send()


def per_device(rng_count, chans, snapshots, train_gates, guard_keep, beam_cells):
    groups, _, span, width = snapshots.shape
    beams = beam_cells.shape[1]
    train_dev = train_gates.shape[1]
    pad = -(-width // LANES) * LANES
    half = span // chans
    lanes = chans * 2 * pad
    store = []
    if 2 * rng_count * train_dev > lanes:
        store = [pltpu.VMEM((lanes, lanes), F32), pltpu.VMEM((lanes, lanes), F32)]
    dma = pltpu.SemaphoreType.DMA
    results = pl.pallas_call(
        functools.partial(kernel, rng_count, chans, pad),
        out_shape=(
            pltpu.VMEM((groups, 2, beams, half), BF16),
            pltpu.VMEM((groups, beams, chans * 2 * width), F32),
        ),
        in_specs=[
            pl.BlockSpec(memory_space=pl.ANY),
            pl.BlockSpec(memory_space=pl.ANY),
            pl.BlockSpec(memory_space=pl.ANY),
            pl.BlockSpec(memory_space=pl.ANY),
        ],
        out_specs=(
            pl.BlockSpec(memory_space=pltpu.VMEM),
            pl.BlockSpec(memory_space=pltpu.VMEM),
        ),
        scratch_shapes=[
            pltpu.VMEM((groups, 2, width, span), BF16),
            pltpu.VMEM((groups, 2, chans, width, half), BF16),
            pltpu.VMEM((groups, train_dev, 2 * pad), BF16),
            pltpu.VMEM((rng_count, chans, train_dev, 2 * pad), BF16),
            pltpu.SMEM(train_gates.shape, jnp.int32),
            pltpu.SMEM(guard_keep.shape, jnp.int32),
            pltpu.SMEM(beam_cells.shape, jnp.int32),
            dma((3,)),
            *store,
            dma((groups,)),
            dma((groups,)),
            dma((groups, chans)),
            dma((groups, chans)),
            dma((rng_count, chans)),
            dma((rng_count, chans)),
            dma,
            dma((groups // chans, chans)),
            dma((groups,)),
        ],
        compiler_params=pltpu.CompilerParams(
            collective_id=0, has_side_effects=True, vmem_limit_bytes=56 * 1024 * 1024
        ),
    )(jnp.transpose(snapshots, (0, 1, 3, 2)), train_gates, guard_keep, beam_cells)
    return pl.pallas_call(
        write_out,
        out_shape=tuple(jax.ShapeDtypeStruct(r.shape, r.dtype) for r in results),
        in_specs=[pl.BlockSpec(memory_space=pltpu.VMEM)] * 2,
        out_specs=(pl.BlockSpec(memory_space=pl.ANY), pl.BlockSpec(memory_space=pl.ANY)),
        scratch_shapes=[dma((2,))],
        compiler_params=pltpu.CompilerParams(vmem_limit_bytes=4 * 1024 * 1024),
    )(*results)


def write_out(beams_in, weights_in, beams_out, weights_out, sem):
    copies = [
        pltpu.make_async_copy(beams_in, beams_out, sem.at[0]),
        pltpu.make_async_copy(weights_in, weights_out, sem.at[1]),
    ]
    for copy in copies:
        copy.start()
    for copy in copies:
        copy.wait()


def solution(mesh):
    placed = (
        P("parts", None, "rng", "chan"),
        P("parts", "rng"),
        P("parts", "rng"),
        P("parts", None),
    )
    return jax.shard_map(
        functools.partial(per_device, mesh.shape["rng"], mesh.shape["chan"]),
        mesh=mesh,
        in_specs=placed,
        out_specs=(P("parts", None, None, ("rng", "chan")), P("parts", None, None)),
        check_vma=False,
    )
```
